8 devices in a mesh: replica: 2 (over z, y), model: 4 (over x, core).
Axes of the slice: x: 2, y: 2, z: 1, core: 2. Of those that a mesh axis runs over, the one named last changes fastest.
Arguments:
- x: bfloat16 [512, 2048], P('replica'), parts along dimension 0
- w_query: bfloat16 [2048, 2048], P(None, 'model')
- w_key: bfloat16 [2048, 128], replicated
- w_value: bfloat16 [2048, 128], replicated
- w_out: bfloat16 [2048, 2048], P('model')
- k_cache: bfloat16 [512, 1, 4096, 128], P('replica'), parts along dimension 0
- v_cache: bfloat16 [512, 1, 4096, 128], P('replica'), parts along dimension 0
- lengths: int32 [512], P('replica'), parts along dimension 0
Outputs:
- output 1: bfloat16 [512, 2048], P('replica'), parts along dimension 0
- output 2: bfloat16 [512, 1, 128], P('replica'), parts along dimension 0
- output 3: bfloat16 [512, 1, 128], P('replica'), parts along dimension 0
There are 2 independent parts. The reference program is written for one: setup_inputs(seed, part) draws one part's arguments, and reference() takes and returns one part's arrays. A program takes and returns all parts, laid end to end along the dimension named above; an argument that names none is the same for every part.
All inputs are finite; a program needn't handle non-finite values.
Results may differ from the reference program's by a relative error of at most 0.00377298.
Values are sent between devices in bfloat16 or wider.
A program may use at most 2.25 GiB of HBM per device.

```python
import jax
import jax.numpy as jnp
from jax import lax

D_MODEL = 2048
NUM_HEADS = 16
KV_HEADS = 1
HEAD_DIM = 128
BATCH_SIZE = 256
CONTEXT_LEN = 4096


def draw_lengths(rng_key):
    key_perm, key_long, key_short = jax.random.split(rng_key, 3)
    perm_rank = jax.random.permutation(key_perm, BATCH_SIZE)
    long_count = max(1, BATCH_SIZE // 16)
    long_len = jax.random.randint(key_long, (BATCH_SIZE,), CONTEXT_LEN // 2, CONTEXT_LEN)
    short_len = jax.random.randint(key_short, (BATCH_SIZE,), 1, 33)
    seq_lens = jnp.where(perm_rank < 2 + long_count, long_len, short_len)
    seq_lens = jnp.where(perm_rank == 1, 1, seq_lens)
    seq_lens = jnp.where(perm_rank == 0, CONTEXT_LEN - 1, seq_lens)
    return seq_lens.astype(jnp.int32)


def setup_inputs(seed: int = 0, part: int = 0) -> dict:
    base_key = jax.random.key(seed)
    key_wq, key_wk, key_wv, key_wo = jax.random.split(base_key, 4)
    part_key = jax.random.fold_in(jax.random.key(seed + 1), part)
    key_x, key_kc, key_vc, key_mean, key_len = jax.random.split(part_key, 5)
    q_width = NUM_HEADS * HEAD_DIM
    kv_width = KV_HEADS * HEAD_DIM
    cache_shape = (BATCH_SIZE, KV_HEADS, CONTEXT_LEN, HEAD_DIM)
    x = jax.random.normal(key_x, (BATCH_SIZE, D_MODEL), jnp.float32).astype(jnp.bfloat16)
    w_query = (jax.random.normal(key_wq, (D_MODEL, q_width), jnp.float32) * D_MODEL ** -0.5).astype(jnp.bfloat16)
    w_key = (jax.random.normal(key_wk, (D_MODEL, kv_width), jnp.float32) * D_MODEL ** -0.5).astype(jnp.bfloat16)
    w_value = (jax.random.normal(key_wv, (D_MODEL, kv_width), jnp.float32) * D_MODEL ** -0.5).astype(jnp.bfloat16)
    w_out = (jax.random.normal(key_wo, (q_width, D_MODEL), jnp.float32) * q_width ** -0.5).astype(jnp.bfloat16)
    k_cache = (1.25 * jax.random.normal(key_kc, cache_shape, jnp.float32)).astype(jnp.bfloat16)
    v_mean = jax.random.normal(key_mean, (BATCH_SIZE, KV_HEADS, 1, HEAD_DIM), jnp.float32)
    v_cache = (jax.random.normal(key_vc, cache_shape, jnp.float32) + v_mean).astype(jnp.bfloat16)
    lengths = draw_lengths(key_len)
    return {"x": x, "w_query": w_query, "w_key": w_key, "w_value": w_value, "w_out": w_out, "k_cache": k_cache, "v_cache": v_cache, "lengths": lengths}


def reference(x, w_query, w_key, w_value, w_out, k_cache, v_cache, lengths):
    group_size = NUM_HEADS // KV_HEADS
    inv_sqrt = HEAD_DIM ** -0.5
    q_all = jnp.dot(x, w_query, preferred_element_type=jnp.float32).astype(jnp.bfloat16)
    k_new = jnp.dot(x, w_key, preferred_element_type=jnp.float32).astype(jnp.bfloat16).reshape(BATCH_SIZE, KV_HEADS, HEAD_DIM)
    v_new = jnp.dot(x, w_value, preferred_element_type=jnp.float32).astype(jnp.bfloat16).reshape(BATCH_SIZE, KV_HEADS, HEAD_DIM)
    q_heads = q_all.reshape(BATCH_SIZE, KV_HEADS, group_size, HEAD_DIM)
    positions = jnp.arange(CONTEXT_LEN)

    def one_sequence(item):
        q_seq, k_rows, v_rows, k_one, v_one, seq_len = item
        q_f32 = q_seq.astype(jnp.float32)
        scores = jnp.einsum("grd,gtd->grt", q_f32, k_rows.astype(jnp.float32)) * inv_sqrt
        score_new = jnp.einsum("grd,gd->gr", q_f32, k_one.astype(jnp.float32)) * inv_sqrt
        in_range = positions[None, None, :] < seq_len
        scores = jnp.where(in_range, scores, -jnp.inf)
        row_max = jnp.maximum(jnp.max(scores, axis=-1), score_new)
        weights = jnp.exp(scores - row_max[:, :, None])
        weight_new = jnp.exp(score_new - row_max)
        norm_sum = jnp.sum(weights, axis=-1) + weight_new
        out_sum = jnp.einsum("grt,gtd->grd", weights.astype(jnp.bfloat16).astype(jnp.float32), v_rows.astype(jnp.float32))
        out_sum = out_sum + weight_new.astype(jnp.bfloat16).astype(jnp.float32)[:, :, None] * v_one.astype(jnp.float32)[:, None, :]
        return (out_sum / norm_sum[:, :, None]).astype(jnp.bfloat16)

    attn_out = lax.map(one_sequence, (q_heads, k_cache, v_cache, k_new, v_new, lengths))
    o_flat = attn_out.reshape(BATCH_SIZE, NUM_HEADS * HEAD_DIM)
    y = (x.astype(jnp.float32) + jnp.dot(o_flat, w_out, preferred_element_type=jnp.float32)).astype(jnp.bfloat16)
    return (y, k_new, v_new)
```

```python
import functools

import jax
import jax.numpy as jnp
from jax import lax
from jax.experimental import pallas as pl
from jax.experimental.pallas import tpu as pltpu
from jax.sharding import PartitionSpec as P

MESH = pl.DeviceIdType.MESH
F32 = jnp.float32
BF16 = jnp.bfloat16
NEG = float("-inf")

BATCH = 256
HALF = 128
DIM = 128
LONG_ROWS = 32
SHORT_ROWS = HALF - LONG_ROWS
FIRST = 32
BLOCK = 512


def nt_dot(a, b):
    return lax.dot_general(a, b, (((1,), (1,)), ((), ())), preferred_element_type=F32)


def dot(a, b):
    return jnp.dot(a, b, preferred_element_type=F32)


def order_tables(lens_row):
    i_sub = lax.broadcasted_iota(jnp.int32, (BATCH, BATCH), 0)
    i_lane = lax.broadcasted_iota(jnp.int32, (BATCH, BATCH), 1)
    row = jnp.broadcast_to(lens_row, (BATCH, BATCH))
    col = jnp.sum(jnp.where(i_sub == i_lane, row, 0.0), axis=1, keepdims=True)
    ahead = (col > row) | ((col == row) & (i_sub < i_lane))
    ahead = jnp.where(ahead, 1.0, 0.0)
    rank_row = jnp.sum(ahead, axis=0, keepdims=True).astype(jnp.int32)
    rank_col = (BATCH - 1) - jnp.sum(ahead, axis=1, keepdims=True).astype(jnp.int32)

    def place(rank):
        slot = rank >> 1
        return ((rank + slot) & 1) * HALF + slot

    return place(rank_row), place(rank_col), col


def project_kernel(x_hbm, wq_hbm, wk_hbm, wv_hbm, lens_ref,
                   q_out, kn_out, vn_out, kp_out, vp_out, meta_out, lenc_out, perm_out, back_out,
                   xv, wqv, wkv, qv, send_buf, sems, ssem, rsem):
    m = lax.axis_index("model")
    r = lax.axis_index("replica")
    core = m % 2
    sib = m + 1 - 2 * core
    depth = x_hbm.shape[1]
    parts = 4
    step = depth // parts
    loads = []
    for i in range(parts):
        cut = pl.ds(i * step, step)
        a = pltpu.make_async_copy(x_hbm.at[:, cut], xv.at[:, cut], sems.at[2 * i])
        b = pltpu.make_async_copy(wq_hbm.at[cut, :], wqv.at[cut, :], sems.at[2 * i + 1])
        a.start()
        b.start()
        loads.append((a, b))
    lk = pltpu.make_async_copy(wk_hbm, wkv.at[:, pl.ds(0, DIM)], sems.at[2 * parts])
    lv = pltpu.make_async_copy(wv_hbm, wkv.at[:, pl.ds(DIM, DIM)], sems.at[2 * parts + 1])
    lk.start()
    lv.start()
    barrier = pltpu.get_barrier_semaphore()
    pl.semaphore_signal(barrier, inc=1, device_id=(r, sib), device_id_type=MESH)
    pl.semaphore_wait(barrier, 1)

    pos_row, pos_col, len_col = order_tables(lens_ref[...].astype(F32))
    p_iota = lax.broadcasted_iota(jnp.int32, (HALF, BATCH), 0)
    own = jnp.where(p_iota + core * HALF == pos_row, 1.0, 0.0)
    own_bf = own.astype(BF16)
    oth_bf = jnp.where(p_iota + (1 - core) * HALF == pos_row, 1.0, 0.0).astype(BF16)
    perm_out[...] = jnp.where(
        lax.broadcasted_iota(jnp.int32, (BATCH, BATCH), 0) == pos_row, 1.0, 0.0).astype(BF16)
    back_out[...] = jnp.where(
        lax.broadcasted_iota(jnp.int32, (BATCH, BATCH), 1) == pos_col, 1.0, 0.0).astype(BF16)
    own_t = lax.broadcasted_iota(jnp.int32, (BATCH, HALF), 1) + core * HALF == pos_col
    i_col = lax.broadcasted_iota(jnp.int32, (BATCH, HALF), 0).astype(F32)
    meta_out[...] = jnp.zeros_like(meta_out)
    meta_out[0:1, :] = jnp.sum(jnp.where(own_t, i_col, 0.0), axis=0, keepdims=True).astype(jnp.int32)
    meta_out[1:2, :] = jnp.sum(jnp.where(own_t, len_col, 0.0), axis=0, keepdims=True).astype(jnp.int32)
    own_len = jnp.sum(own * lens_ref[...].astype(F32), axis=1, keepdims=True)
    lenc_out[...] = jnp.broadcast_to(own_len, (HALF, DIM)).astype(jnp.int32)

    acc = None
    for i in range(parts):
        loads[i][0].wait()
        loads[i][1].wait()
        cut = pl.ds(i * step, step)
        t = dot(xv[:, cut], wqv[cut, :])
        acc = t if acc is None else acc + t
    qv[...] = acc.astype(BF16)
    q_oth = dot(oth_bf, qv[...]).astype(BF16)
    for h in range(4):
        send_buf[h] = q_oth[:, h * DIM:(h + 1) * DIM]
    push = pltpu.make_async_remote_copy(
        src_ref=send_buf, dst_ref=q_out.at[pl.ds(4, 4)], send_sem=ssem, recv_sem=rsem,
        device_id=(r, sib), device_id_type=MESH)
    push.start()
    q_own = dot(own_bf, qv[...]).astype(BF16)
    for h in range(4):
        q_out[h] = q_own[:, h * DIM:(h + 1) * DIM]
    lk.wait()
    lv.wait()
    kv = dot(xv[...], wkv[...]).astype(BF16)
    kn_out[...] = kv[:, :DIM]
    vn_out[...] = kv[:, DIM:]
    kv_own = dot(own_bf, kv)
    kp_out[...] = kv_own[:, :DIM]
    vp_out[...] = kv_own[:, DIM:]
    push.wait()


def attend_kernel(j0, rows, slots, meta, q_ref, kp, vp, lenc, kc, vc, w_own, w_sib, _order,
                  mine_out, send_out,
                  qf, kfirst, vfirst, kb, vb, wv, osc, asem, bsem, wsem):
    m = lax.axis_index("model")
    chip = m // 2
    scale = DIM ** -0.5

    def first_copies(j, _):
        src = meta[0, j0 + j]
        at = pl.ds(pl.multiple_of(j * FIRST, FIRST), FIRST)
        pltpu.make_async_copy(kc.at[src, 0, pl.ds(0, FIRST), :], kfirst.at[at, :], asem.at[0]).start()
        pltpu.make_async_copy(vc.at[src, 0, pl.ds(0, FIRST), :], vfirst.at[at, :], asem.at[1]).start()
        return 0

    lax.fori_loop(0, rows, first_copies, 0)

    def blocks_of(j):
        return (meta[1, j0 + j] + (BLOCK - 1)) // BLOCK

    def issue(j):
        src = meta[0, j0 + j]
        slot = j % slots

        def one(cache, buf, sem):
            def go(b, _):
                at = pl.ds(pl.multiple_of(b * BLOCK, BLOCK), BLOCK)
                pltpu.make_async_copy(cache.at[src, 0, at, :], buf.at[slot, at, :], sem).start()
                return 0
            lax.fori_loop(0, blocks_of(j), go, 0)

        one(kc, kb, bsem.at[0, slot])
        one(vc, vb, bsem.at[1, slot])

    n_long = lax.fori_loop(
        0, rows, lambda j, n: n + jnp.where(meta[1, j0 + j] > FIRST, 1, 0), jnp.int32(0))

    def prime(j, _):
        issue(j)
        return 0

    lax.fori_loop(0, jnp.minimum(n_long, slots), prime, 0)
    wo = pltpu.make_async_copy(w_own, wv.at[pl.ds(0, 512), :], wsem.at[0])
    ws = pltpu.make_async_copy(w_sib, wv.at[pl.ds(512, 512), :], wsem.at[1])
    wo.start()
    ws.start()

    for h in range(8):
        qf[h * HALF:(h + 1) * HALF, :] = q_ref[h].astype(F32)

    pltpu.make_async_copy(kfirst, kfirst, asem.at[0]).wait()
    pltpu.make_async_copy(vfirst, vfirst, asem.at[1]).wait()
    lane = lax.broadcasted_iota(jnp.int32, (64, 256), 1)
    sub = lax.broadcasted_iota(jnp.int32, (64, 256), 0)
    same = (lane // FIRST) == (sub % 8)
    tok = lane % FIRST
    for g in range(rows // 8):
        a = j0 + g * 8
        q = jnp.concatenate([qf[h * HALF + a:h * HALF + a + 8, :] for h in range(8)], axis=0)
        kn = jnp.concatenate([kp[a:a + 8, :]] * 8, axis=0)
        vn = jnp.concatenate([vp[a:a + 8, :]] * 8, axis=0)
        ln = jnp.concatenate([jnp.concatenate([lenc[a:a + 8, :]] * 8, axis=0)] * 2, axis=1)
        at = slice(g * 256, (g + 1) * 256)
        s = nt_dot(q.astype(BF16), kfirst[at, :]) * scale
        s = jnp.where(same & (tok < ln), s, NEG)
        sn = jnp.sum(q * kn, axis=1, keepdims=True) * scale
        top = jnp.maximum(jnp.max(s, axis=1, keepdims=True), sn)
        e = jnp.exp(s - top)
        en = jnp.exp(sn - top)
        tot = jnp.sum(e, axis=1, keepdims=True) + en
        num = dot(e.astype(BF16), vfirst[at, :]) + en.astype(BF16).astype(F32) * vn
        o = num / tot
        for h in range(8):
            osc[h * rows + g * 8:h * rows + g * 8 + 8, :] = o[h * 8:(h + 1) * 8, :]

    def row_body(j, slot, length, n):
        q8 = qf[pl.ds(j0 + j, 8, stride=HALF), :]
        zero = jnp.zeros_like(q8)
        qq = jnp.concatenate(
            [jnp.concatenate([q8, zero], axis=1), jnp.concatenate([zero, q8], axis=1)], axis=0).astype(BF16)
        kn = kp[pl.ds(j0 + j, 1), :]
        vn = vp[pl.ds(j0 + j, 1), :]
        sn = jnp.sum(q8 * kn, axis=1, keepdims=True) * scale
        lane = lax.broadcasted_iota(jnp.int32, (16, BLOCK), 1)
        sub = lax.broadcasted_iota(jnp.int32, (16, BLOCK), 0)
        tok = lane + jnp.where(sub >= 8, BLOCK, 0)
        scores = []
        for b in range(n):
            at = 2 * b * BLOCK
            k2 = jnp.concatenate([kb[slot, at:at + BLOCK, :], kb[slot, at + BLOCK:at + 2 * BLOCK, :]], axis=1)
            s = nt_dot(qq, k2) * scale
            scores.append(jnp.where(tok + at < length, s, NEG))
        top = functools.reduce(jnp.maximum, scores)
        top = jnp.max(top, axis=1, keepdims=True)
        top = jnp.maximum(jnp.maximum(top[:8], top[8:]), sn)
        top2 = jnp.concatenate([top, top], axis=0)
        es = [jnp.exp(s - top2) for s in scores]
        tot = jnp.sum(functools.reduce(jnp.add, es), axis=1, keepdims=True)
        num = None
        for b in range(n):
            at = 2 * b * BLOCK
            v2 = jnp.concatenate([vb[slot, at:at + BLOCK, :], vb[slot, at + BLOCK:at + 2 * BLOCK, :]], axis=1)
            t = dot(es[b].astype(BF16), v2)
            num = t if num is None else num + t
        en = jnp.exp(sn - top)
        num = num[:8, :DIM] + num[8:, DIM:] + en.astype(BF16).astype(F32) * vn
        tot = tot[:8] + tot[8:] + en
        osc[pl.ds(j, 8, stride=rows), :] = num / tot

    def long_row(j, _):
        slot = j % slots
        length = meta[1, j0 + j]
        nb = blocks_of(j)

        def done(cache, buf, sem):
            def go(b, _):
                at = pl.ds(0, BLOCK)
                pltpu.make_async_copy(cache.at[0, 0, at, :], buf.at[slot, at, :], sem).wait()
                return 0
            lax.fori_loop(0, nb, go, 0)

        done(kc, kb, bsem.at[0, slot])
        done(vc, vb, bsem.at[1, slot])

        @pl.when(nb % 2 == 1)
        def _():
            at = pl.ds(pl.multiple_of(nb * BLOCK, BLOCK), BLOCK)
            kb[slot, at, :] = jnp.zeros((BLOCK, DIM), BF16)
            vb[slot, at, :] = jnp.zeros((BLOCK, DIM), BF16)

        pairs = (nb + 1) // 2
        for n in range(1, 5):
            @pl.when(pairs == n)
            def _(n=n):
                row_body(j, slot, length, n)

        @pl.when(j + slots < n_long)
        def _():
            issue(j + slots)
        return 0

    lax.fori_loop(0, n_long, long_row, 0)

    wo.wait()
    ws.wait()
    part = rows // 2

    def halves(h, which):
        return osc[pl.ds(h * rows + which * part, part), :]

    o = jnp.concatenate(
        [jnp.concatenate([halves(h, chip), halves(h, 1 - chip)], axis=0) for h in range(8)],
        axis=1).astype(BF16)
    for c in range(4):
        cut = slice(c * 512, (c + 1) * 512)
        res = dot(o, wv[:, cut])
        mine_out[:, cut] = res[:part]
        send_out[:, cut] = res[part:]


def combine_kernel(p1, r1, p2, s2, x_ref, perm, y, r2, ssem, rsem):
    m = lax.axis_index("model")
    r = lax.axis_index("replica")
    chip = m // 2
    core = m % 2
    sib = m + 1 - 2 * core
    far = (m + 2) % 4
    barrier = pltpu.get_barrier_semaphore()
    for other in (sib, far):
        pl.semaphore_signal(barrier, inc=1, device_id=(r, other), device_id_type=MESH)
    pl.semaphore_wait(barrier, 2)

    def place(which, f, c=core):
        n = (SHORT_ROWS if which == 0 else LONG_ROWS) // 2
        base = (LONG_ROWS if which == 0 else 0)
        return pl.ds(pl.multiple_of(c * HALF + base + f * n, 16), n)

    def push(src, dst, i, dev):
        c = pltpu.make_async_remote_copy(
            src_ref=src, dst_ref=dst, send_sem=ssem.at[i], recv_sem=rsem.at[i],
            device_id=(r, dev), device_id_type=MESH)
        c.start()
        return c

    sends = [push(s2, r2, 0, far)]

    def finish(which, mine, got):
        at = place(which, chip)
        xs = dot(perm[at, :], x_ref[...])
        y[at, :] = (xs + (mine + got)).astype(BF16)

    finish(0, p1[...], r1[...])
    mine1 = place(0, chip)
    far1 = push(y.at[mine1, :], y.at[mine1, :], 1, far)
    sib1 = push(y.at[mine1, :], y.at[mine1, :], 2, sib)
    sends[0].wait_recv()
    finish(1, p2[...], r2[...])
    mine2 = place(1, chip)
    far2 = push(y.at[mine2, :], y.at[mine2, :], 3, far)
    sib2 = push(y.at[mine2, :], y.at[mine2, :], 4, sib)
    far1.wait_recv()
    got1 = place(0, 1 - chip)
    fwd1 = push(y.at[got1, :], y.at[got1, :], 5, sib)
    far2.wait_recv()
    got2 = place(1, 1 - chip)
    fwd2 = push(y.at[got2, :], y.at[got2, :], 6, sib)
    for c in (sib1, sib2, fwd1, fwd2):
        c.wait_recv()
    for c in (sends[0], far1, sib1, far2, sib2, fwd1, fwd2):
        c.wait_send()


def cost(us):
    return pl.CostEstimate(flops=int(us * 3e8), bytes_accessed=int(us * 2e6), transcendentals=0)


VM = pl.BlockSpec(memory_space=pltpu.VMEM)
SM = pl.BlockSpec(memory_space=pltpu.SMEM)
ANY = pl.BlockSpec(memory_space=pl.ANY)


def sds(shape, dtype):
    return jax.ShapeDtypeStruct(shape, dtype)


def attend_call(j0, rows, slots, us, *args):
    part = rows // 2
    return pl.pallas_call(
        functools.partial(attend_kernel, j0, rows, slots),
        out_shape=(sds((part, 2048), F32), sds((part, 2048), F32)),
        in_specs=[SM, VM, VM, VM, VM, ANY, ANY, ANY, ANY, ANY],
        out_specs=(VM, VM),
        scratch_shapes=[
            pltpu.VMEM((8 * HALF, DIM), F32),
            pltpu.VMEM((rows * FIRST, DIM), BF16),
            pltpu.VMEM((rows * FIRST, DIM), BF16),
            pltpu.VMEM((slots, 4096, DIM), BF16),
            pltpu.VMEM((slots, 4096, DIM), BF16),
            pltpu.VMEM((1024, 2048), BF16),
            pltpu.VMEM((8 * rows, DIM), F32),
            pltpu.SemaphoreType.DMA((2,)),
            pltpu.SemaphoreType.DMA((2, slots)),
            pltpu.SemaphoreType.DMA((2,)),
        ],
        compiler_params=pltpu.CompilerParams(vmem_limit_bytes=32 * 1024 * 1024),
        cost_estimate=cost(us),
        name=f"attend_{j0}",
    )(*args)


def local_step(x, w_query, w_key, w_value, w_out, k_cache, v_cache, lengths):
    swap = [(i, i ^ 1) for i in range(4)]
    cross = [(i, i ^ 2) for i in range(4)]
    w_sib = lax.ppermute(w_out, "model", swap)
    q, k_new, v_new, kp, vp, meta, lenc, perm, back = pl.pallas_call(
        project_kernel,
        out_shape=(
            sds((8, HALF, DIM), BF16), sds((BATCH, DIM), BF16), sds((BATCH, DIM), BF16),
            sds((HALF, DIM), F32), sds((HALF, DIM), F32), sds((8, HALF), jnp.int32),
            sds((HALF, DIM), jnp.int32), sds((BATCH, BATCH), BF16), sds((BATCH, BATCH), BF16),
        ),
        in_specs=[ANY, ANY, ANY, ANY, VM],
        out_specs=(VM,) * 9,
        scratch_shapes=[
            pltpu.VMEM((BATCH, 2048), BF16),
            pltpu.VMEM((2048, 512), BF16),
            pltpu.VMEM((2048, 2 * DIM), BF16),
            pltpu.VMEM((BATCH, 512), BF16),
            pltpu.VMEM((4, HALF, DIM), BF16),
            pltpu.SemaphoreType.DMA((10,)),
            pltpu.SemaphoreType.DMA,
            pltpu.SemaphoreType.DMA,
        ],
        compiler_params=pltpu.CompilerParams(
            collective_id=0, has_side_effects=True, vmem_limit_bytes=24 * 1024 * 1024),
        cost_estimate=cost(5),
        name="project",
    )(x, w_query, w_key, w_value, lengths.reshape(1, BATCH))
    common = (meta, q, kp, vp, lenc, k_cache, v_cache, w_out, w_sib)
    p1, s1 = attend_call(LONG_ROWS, SHORT_ROWS, 2, 4, *common, meta)
    r1 = lax.ppermute(s1, "model", cross)
    p2, s2 = attend_call(0, LONG_ROWS, 6, 10, *common, p1)
    y_sorted = pl.pallas_call(
        combine_kernel,
        out_shape=sds((BATCH, 2048), BF16),
        in_specs=[VM] * 6,
        out_specs=VM,
        scratch_shapes=[
            pltpu.VMEM((LONG_ROWS // 2, 2048), F32),
            pltpu.SemaphoreType.DMA((7,)),
            pltpu.SemaphoreType.DMA((7,)),
        ],
        compiler_params=pltpu.CompilerParams(
            collective_id=1, has_side_effects=True, vmem_limit_bytes=24 * 1024 * 1024),
        cost_estimate=cost(10),
        name="combine",
    )(p1, r1, p2, s2, x, perm)
    y = jnp.dot(back, y_sorted, preferred_element_type=F32).astype(BF16)
    return y, k_new.reshape(BATCH, 1, DIM), v_new.reshape(BATCH, 1, DIM)


def solution(mesh):
    rows_spec = P("replica")
    return jax.shard_map(
        local_step,
        mesh=mesh,
        in_specs=(P("replica", None), P(None, "model"), P(), P(), P("model", None), rows_spec, rows_spec, rows_spec),
        out_specs=(rows_spec, rows_spec, rows_spec),
        check_vma=False,
    )
```
